32 devices in a mesh: grp: 2 (over x), src: 8 (over z, y), tgt: 2 (over core).
Axes of the slice: x: 2, y: 2, z: 4, core: 2. Of those that a mesh axis runs over, the one named last changes fastest.
Arguments:
- densities: bfloat16 [512, 32768], P('grp', ('src', 'tgt')), parts along dimension 0, may hold values from -6 to 6
- compress: bfloat16 [65536, 2, 256], P(('grp', 'src', 'tgt')), parts along dimension 0, may hold values from -0.0625 to 0.0625
- level_a: bfloat16 [6, 2048, 2, 256], P('grp', 'src', None, 'tgt'), parts along dimension 0, may hold values from -0.1875 to 0.1875
- level_b: bfloat16 [6, 2048, 2, 256], P('grp', 'src', None, 'tgt'), parts along dimension 0, may hold values from -0.1875 to 0.1875
- expand: bfloat16 [4096, 2, 4096], P(('grp', 'src'), None, 'tgt'), parts along dimension 0, may hold values from -0.25 to 0.25
- near_tiles: bfloat16 [2048, 128, 2, 128], P(('grp', 'src', 'tgt')), parts along dimension 0, may hold values from -0.375 to 0.375
- tile_pairs: int32 [2048, 2], P(('grp', 'src', 'tgt')), parts along dimension 0, may hold values from 0 to 15
- tile_count: int32 [32], P(('grp', 'src', 'tgt')), parts along dimension 0, may hold values from 1 to 63, as said below
- cluster_order: int32 [32, 16], P(('grp', 'src', 'tgt')), parts along dimension 0, may hold values from 0 to 15, each once within a row
Outputs:
- potential: bfloat16 [512, 32768], P('grp', ('src', 'tgt')), parts along dimension 0
The draws below stay inside these ranges and needn't reach their ends.
There are 2 independent parts, one for each index of `grp`. The reference program is written for one: setup_inputs(seed, part) draws one part's arguments, and reference() takes and returns one part's arrays. A program takes and returns all parts, laid end to end along the dimension named above; each array names one. Nothing has to cross between parts.
Inputs may be any that keep to these rules, and one draw needn't show every extreme that they name: For every i below 8, tile_count[i] + tile_count[i + 8] == 64; slots at or beyond a device's count are unused. `cluster_order`: each row is a permutation.
All inputs are finite; a program needn't handle non-finite values.
Results may differ from the reference program's by a relative error of at most 0.007.
Values may be sent and summed in bfloat16 or wider, within the bound.
A program may use at most 128 MiB of HBM per device.

```python
import jax
import jax.numpy as jnp
from jax import lax

RHS = 128
K = 256
PC = 128
MAXT = 64
PTS = 2048
CL = 16
SHARDS = 16
PTS_ALL = 32768
LEVELS = 3
N_SRC = 8
N_TGT = 2


def draw_tile_count(key, part):
    src_total = SHARDS // N_TGT
    halfway = src_total // 2
    first_key, second_key = jax.random.split(jax.random.fold_in(key, 17))
    heavy = jax.random.randint(first_key, (halfway, N_TGT), MAXT // 2, MAXT)
    heavy = heavy.at[0, 0].set(MAXT - 1)
    light = MAXT - heavy
    flipped = jax.random.randint(second_key, (halfway, N_TGT), 0, 2)
    lower = jnp.where(flipped == 1, heavy, light)
    upper = jnp.where(flipped == 1, light, heavy)
    return jnp.concatenate([lower, upper], axis=0).reshape(SHARDS).astype(jnp.int32)


def set_ends(drawn, rng, low, top_value):
    dims = drawn.shape
    spot = [jax.random.randint(jax.random.fold_in(rng, axis), (), 0, dims[axis]) for axis in range(len(dims))]
    drawn = drawn.at[tuple(spot)].set(low)
    longest = dims.index(max(dims))
    spot[longest] = (spot[longest] + 1) % dims[longest]
    return drawn.at[tuple(spot)].set(top_value)


def level_of(key, shape, cuts, least, largest):
    factor_of, own = 1.0, jax.random.fold_in(key, 6)
    for axis_at, shards_of in cuts:
        heights = jnp.exp(jax.random.uniform(jax.random.fold_in(own, axis_at), (shards_of,), jnp.float32, least / len(cuts), largest / len(cuts)))
        factor_of = factor_of * jnp.repeat(heights, shape[axis_at] // shards_of).reshape([-1 if axis == axis_at else 1 for axis in range(len(shape))])
    return factor_of


def gaussian(key, extent, scale, limit, cuts=(), held_as=jnp.bfloat16):
    gain = level_of(key, extent, cuts, -0.22, 0.18) if cuts else 1.0
    result = jax.random.normal(key, extent, jnp.float32) * scale * gain
    return jnp.minimum(jnp.maximum(result, -limit), limit).astype(held_as)


def setup_inputs(seed: int = 0, part: int = 0) -> dict:
    key_of = jax.random.split(jax.random.key(seed), 10)
    part_splits = jax.random.split(jax.random.fold_in(key_of[9], part), 10)
    return {
        "densities": gaussian(part_splits[0], (2 * RHS, PTS_ALL), 1.0, 6.0, ((1, 16),)),
        "compress": gaussian(part_splits[1], (PTS_ALL, 2, K), (2 * N_TGT * PTS) ** -0.5, 0.0625, ((0, 16),)),
        "level_a": gaussian(part_splits[2], (LEVELS, N_SRC * K, 2, K), (4 * K) ** -0.5, 0.1875, ((1, 8), (3, 2))),
        "level_b": gaussian(part_splits[3], (LEVELS, N_SRC * K, 2, K), (4 * K) ** -0.5, 0.1875, ((1, 8), (3, 2))),
        "expand": gaussian(part_splits[4], (N_SRC * K, 2, N_TGT * PTS), (2 * K) ** -0.5, 0.25, ((0, 8), (2, 2))),
        "near_tiles": gaussian(part_splits[5], (SHARDS * MAXT, PC, 2, PC), (2 * PC) ** -0.5, 0.375, ((0, 16),)),
        "tile_pairs": set_ends(jax.random.randint(part_splits[6], (SHARDS * MAXT, 2), 0, CL), jax.random.fold_in(part_splits[6], 1), 0, CL - 1).astype(jnp.int32),
        "tile_count": draw_tile_count(jax.random.fold_in(jax.random.fold_in(key_of[9], part), 71), part),
        "cluster_order": jax.vmap(lambda own: jax.random.permutation(own, CL))(jax.random.split(part_splits[8], SHARDS)).reshape((SHARDS, CL)).astype(jnp.int32),
    }


def complex_product(operand, matrix):
    product = jnp.dot(operand, matrix, preferred_element_type=jnp.float32)
    half_rows = operand.shape[0] // 2
    half_cols = matrix.shape[1] // 2
    real_part = product[:half_rows, :half_cols] - product[half_rows:, half_cols:]
    imag_part = product[:half_rows, half_cols:] + product[half_rows:, :half_cols]
    return jnp.concatenate([real_part, imag_part], axis=0)


def near_sum(sources, tile_blocks, source_ids, target_ids, active, targets):
    half_rows = sources.shape[0] // 2
    cluster_size = tile_blocks.shape[1]
    picked = jnp.take(sources, source_ids, axis=1).astype(jnp.float32)
    product = jnp.einsum("rjp,jpq->rjq", picked, tile_blocks.astype(jnp.float32), precision=lax.Precision.HIGHEST)
    real_part = product[:half_rows, :, :cluster_size] - product[half_rows:, :, cluster_size:]
    imag_part = product[:half_rows, :, cluster_size:] + product[half_rows:, :, :cluster_size]
    joined = jnp.concatenate([real_part, imag_part], axis=0)
    chooser = ((target_ids[:, None] == jnp.arange(targets, dtype=jnp.int32)[None, :]) & active[:, None]).astype(jnp.float32)
    return jnp.einsum("rjq,jc->rcq", joined, chooser, precision=lax.Precision.HIGHEST)


def reference(densities, compress, level_a, level_b, expand, near_tiles, tile_pairs, tile_count, cluster_order):
    row_count = densities.shape[0]
    shard_dens = densities.reshape(row_count, SHARDS, PTS).transpose(1, 0, 2)
    shard_comp = compress.reshape(SHARDS, PTS, 2 * K)

    def compress_one(items):
        return complex_product(items[0], items[1])

    partial_value = lax.map(compress_one, (shard_dens, shard_comp))
    coefficients = jnp.sum(partial_value.reshape(N_SRC, N_TGT, row_count, K), axis=1).astype(jnp.bfloat16)
    full_a = level_a.reshape(LEVELS, N_SRC, K, 2 * K)
    full_b = level_b.reshape(LEVELS, N_SRC, K, 2 * K)

    def level_one(items):
        summed = complex_product(items[0], items[2]) + complex_product(items[1], items[3])
        return summed.astype(jnp.bfloat16)

    for level_index in range(LEVELS):
        partner_index = jnp.bitwise_xor(jnp.arange(N_SRC, dtype=jnp.int32), 1 << level_index)
        partner_coeff = coefficients[partner_index]
        coefficients = lax.map(level_one, (coefficients, partner_coeff, full_a[level_index], full_b[level_index]))

    shard_coeff = jnp.repeat(coefficients, N_TGT, axis=0)
    shard_expand = expand.reshape(N_SRC, K, 2, N_TGT, PTS).transpose(0, 3, 1, 2, 4).reshape(SHARDS, K, 2 * PTS)
    shard_tiles = near_tiles.reshape(SHARDS, MAXT, PC, 2 * PC)
    shard_pairs = tile_pairs.reshape(SHARDS, MAXT, 2)

    def finish_one(items):
        dens, coeff, expansion, tile_blocks, pairs, count, order = items
        far_field = complex_product(coeff, expansion).reshape(row_count, CL, PC)
        placed = jnp.zeros((row_count, CL, PC), jnp.float32).at[:, order, :].set(far_field)
        active = jnp.arange(MAXT, dtype=jnp.int32) < count
        near_field = near_sum(dens.reshape(row_count, CL, PC), tile_blocks, pairs[:, 1], pairs[:, 0], active, CL)
        return (placed + near_field).reshape(row_count, PTS).astype(jnp.bfloat16)

    results = lax.map(finish_one, (shard_dens, shard_coeff, shard_expand, shard_tiles, shard_pairs, tile_count, cluster_order))
    return results.transpose(1, 0, 2).reshape(row_count, PTS_ALL)
```

```python
import functools

import jax
import jax.numpy as jnp
from jax import lax
from jax.experimental import pallas as pl
from jax.experimental.pallas import tpu as pltpu
from jax.sharding import PartitionSpec as P

MESH = pl.DeviceIdType.MESH
CHUNKS = 2
UNROLL = 4


def lift(real, imag, perm):
    upper = jnp.concatenate([real, -imag], axis=1)
    lower = jnp.concatenate([imag, real], axis=1)
    both = jnp.concatenate([upper, lower], axis=0)
    return jnp.dot(both, perm, preferred_element_type=jnp.float32).astype(jnp.bfloat16)


def flat(block):
    return block.reshape(block.shape[0] * 2, block.shape[2])


def kernel(
    sizes,
    dens_h, comp_h, la_h, lb_h, exp_h, tiles_h, pairs_s, count_s, order_s,
    out_h,
    dens_v, comp_v, lev_v, exp_v, tiles_v, lifted_v, sums_v, part_v, part_r, coef_v, recv_v, fin_v, out_v,
    dens_sem, comp_sem, lev_sem, levs_sem, levr_sem, exp_sem, tiles_sem, part_sem, send_sem, recv_sem, fin_sem, out_sem,
):
    levels, clusters, width, slots, rhs, rank, n_tgt = sizes
    src, tgt = lax.axis_index("src"), lax.axis_index("tgt")
    other = 1 - tgt
    sibling = {"tgt": other}
    partners = [{"src": src ^ (1 << level)} for level in range(levels)]
    lanes = rank // width
    comp_parts = comp_sem.shape[1]
    rows_part = comp_h.shape[0] // comp_parts
    tile_parts = tiles_sem.shape[0]
    slots_part = slots // tile_parts

    loads_dens = pltpu.make_async_copy(dens_h, dens_v, dens_sem)
    loads_dens.start()
    loads_comp = [
        [
            pltpu.make_async_copy(
                comp_h.at[pl.ds(part * rows_part, rows_part), :, pl.ds(lane * width, width)],
                comp_v.at[lane, pl.ds(part * rows_part, rows_part)],
                comp_sem.at[lane, part],
            )
            for lane in range(lanes)
        ]
        for part in range(comp_parts)
    ]
    for part in loads_comp:
        for item in part:
            item.start()
    barrier = pltpu.get_barrier_semaphore()
    for target in [sibling] + partners:
        pl.semaphore_signal(barrier, inc=1, device_id=target, device_id_type=MESH)
    factors = (la_h, lb_h)
    loads_lev = [pltpu.make_async_copy(factors[ab], lev_v.at[ab, tgt], lev_sem.at[ab]) for ab in range(2)]
    for item in loads_lev:
        item.start()
    loads_tiles = [
        pltpu.make_async_copy(
            tiles_h.at[pl.ds(part * slots_part, slots_part)],
            tiles_v.at[pl.ds(part * slots_part, slots_part)],
            tiles_sem.at[part],
        )
        for part in range(tile_parts)
    ]
    for item in loads_tiles:
        item.start()
    loads_exp = [
        pltpu.make_async_copy(exp_h.at[:, :, pl.ds(c * width, width)], exp_v.at[c], exp_sem.at[c])
        for c in range(clusters)
    ]
    for item in loads_exp:
        item.start()

    row = lax.broadcasted_iota(jnp.int32, (2 * width, 2 * width), 0)
    col = lax.broadcasted_iota(jnp.int32, (2 * width, 2 * width), 1)
    spot = jnp.where(row < width, 2 * row, 2 * (row - width) + 1)
    perm = (spot == col).astype(jnp.float32).astype(jnp.bfloat16)

    pl.semaphore_wait(barrier, 1 + levels)
    swaps_lev = [
        pltpu.make_async_remote_copy(
            src_ref=factors[ab], dst_ref=lev_v.at[ab, tgt], send_sem=levs_sem.at[ab], recv_sem=levr_sem.at[ab],
            device_id=sibling, device_id_type=MESH,
        )
        for ab in range(2)
    ]
    for item in swaps_lev:
        item.start()

    loads_dens.wait()
    for c in range(clusters):
        cut = pl.ds(c * width, width)
        lifted_v[c] = lift(dens_v[:rhs, cut], dens_v[rhs:, cut], perm)
    per_part = clusters // comp_parts
    sums = [jnp.zeros((2 * rhs, width), jnp.float32) for _ in range(lanes)]
    for part in range(comp_parts):
        for item in loads_comp[part]:
            item.wait()
        for c in range(part * per_part, (part + 1) * per_part):
            block = lifted_v[c]
            for lane in range(lanes):
                sums[lane] = sums[lane] + jnp.dot(
                    block, flat(comp_v[lane, pl.ds(c * width, width)]), preferred_element_type=jnp.float32
                )
    half = rhs // n_tgt
    for h in range(n_tgt):
        for ri in range(2):
            for lane in range(lanes):
                part_v[h, ri, :, pl.ds(lane * width, width)] = sums[lane][ri * rhs + h * half : ri * rhs + (h + 1) * half]
    swap_part = pltpu.make_async_remote_copy(
        src_ref=part_v.at[other], dst_ref=part_r, send_sem=part_sem.at[0], recv_sem=part_sem.at[1],
        device_id=sibling, device_id_type=MESH,
    )
    swap_part.start()

    rows = half // CHUNKS

    def send(level, q):
        copy = pltpu.make_async_remote_copy(
            src_ref=coef_v.at[level, q], dst_ref=recv_v.at[level, q],
            send_sem=send_sem.at[level, q], recv_sem=recv_sem.at[level, q],
            device_id=partners[level], device_id_type=MESH,
        )
        copy.start()
        return copy

    def lifted(value):
        return jnp.concatenate(
            [
                lift(value[0, :, lane * width : (lane + 1) * width], value[1, :, lane * width : (lane + 1) * width], perm)
                for lane in range(lanes)
            ],
            axis=1,
        )

    def apply(value, ab, level):
        return jnp.concatenate(
            [
                jnp.dot(value, flat(lev_v[ab, h, level]), preferred_element_type=jnp.float32)
                for h in range(n_tgt)
            ],
            axis=1,
        )

    count = count_s[0]
    last = [jnp.int32(slots) for _ in range(clusters)]
    sums_v[slots] = jnp.zeros((2 * rhs, width), jnp.float32)

    def near_step(step, last):
        last = list(last)
        base = step * UNROLL
        terms = [
            jnp.dot(lifted_v[pairs_s[1, base + u]], flat(tiles_v[base + u]), preferred_element_type=jnp.float32)
            for u in range(UNROLL)
        ]
        for u in range(UNROLL):
            slot = base + u
            target = pairs_s[0, slot]
            active = slot < count
            before = jnp.int32(slots)
            for c in range(clusters):
                hit = target == c
                before = jnp.where(hit, last[c], before)
                last[c] = jnp.where(hit & active, slot, last[c])
            sums_v[slot] = terms[u] + sums_v[before]
        return tuple(last)

    swap_part.wait()
    sends = []
    for q in range(CHUNKS):
        cut = pl.ds(q * rows, rows)
        coef_v[0, q] = (part_v[tgt, :, cut, :] + part_r[:, cut, :]).astype(jnp.bfloat16)
        sends.append(send(0, q))
    for item in loads_lev:
        item.wait()
    for item in swaps_lev:
        item.wait()
    current = sends
    done_sends = []
    swaps_fin = []
    tiles_waited = 0
    for level in range(levels):
        own = [apply(lifted(coef_v[level, q]), 0, level) for q in range(CHUNKS)]
        first, final = (tile_parts * level) // levels, (tile_parts * (level + 1)) // levels
        for part in range(first, final):
            loads_tiles[part].wait()
        last = lax.fori_loop(
            first * slots_part // UNROLL, final * slots_part // UNROLL, near_step, tuple(last)
        )
        following = []
        for q in range(CHUNKS):
            current[q].wait_recv()
            total = own[q] + apply(lifted(recv_v[level, q]), 1, level)
            fresh = jnp.stack([total[:rows], total[rows:]]).astype(jnp.bfloat16)
            if level + 1 < levels:
                coef_v[level + 1, q] = fresh
                following.append(send(level + 1, q))
            else:
                fin_v[tgt, q] = fresh
                copy = pltpu.make_async_remote_copy(
                    src_ref=fin_v.at[tgt, q], dst_ref=fin_v.at[tgt, q],
                    send_sem=fin_sem.at[0, q], recv_sem=fin_sem.at[1, q],
                    device_id=sibling, device_id_type=MESH,
                )
                copy.start()
                swaps_fin.append(copy)
        done_sends += current
        current = following
    for item in loads_exp:
        item.wait()
    for item in swaps_fin:
        item.wait()
    for item in done_sends:
        item.wait_send()

    whole = [
        jnp.concatenate([fin_v[h, q, ri] for h in range(n_tgt) for q in range(CHUNKS)], axis=0) for ri in range(2)
    ]
    operand = jnp.concatenate(
        [
            lift(whole[0][:, lane * width : (lane + 1) * width], whole[1][:, lane * width : (lane + 1) * width], perm)
            for lane in range(lanes)
        ],
        axis=1,
    )
    out_parts = out_sem.shape[0]
    per_out = clusters // out_parts
    stores = []
    for part in range(out_parts):
        for t in range(part * per_out, (part + 1) * per_out):
            origin = jnp.int32(0)
            for c in range(clusters):
                origin = jnp.where(order_s[0, c] == t, c, origin)
            far = jnp.dot(operand, flat(exp_v[origin]), preferred_element_type=jnp.float32)
            out_v[:, pl.ds(t * width, width)] = (far + sums_v[last[t]]).astype(jnp.bfloat16)
        cut = pl.ds(part * per_out * width, per_out * width)
        stores.append(pltpu.make_async_copy(out_v.at[:, cut], out_h.at[:, cut], out_sem.at[part]))
        stores[-1].start()
    for item in stores:
        item.wait()


def shards(
    densities, compress, level_a, level_b, expand, near_tiles, tile_pairs, tile_count, cluster_order
):
    row_count, points = densities.shape
    rhs = row_count // 2
    rank = compress.shape[2]
    levels = level_a.shape[0]
    clusters = cluster_order.shape[1]
    width = points // clusters
    slots = near_tiles.shape[0]
    n_tgt = lax.axis_size("tgt")
    sizes = (levels, clusters, width, slots, rhs, rank, n_tgt)
    lanes = rank // width
    rows = rhs // n_tgt // CHUNKS
    comp_parts, tile_parts, out_parts = 4, 16, 4
    bf16, f32 = jnp.bfloat16, jnp.float32
    anywhere = pl.BlockSpec(memory_space=pl.ANY)
    scalar = pl.BlockSpec(memory_space=pltpu.SMEM)
    dma = pltpu.SemaphoreType.DMA
    return pl.pallas_call(
        functools.partial(kernel, sizes),
        out_shape=jax.ShapeDtypeStruct((row_count, points), bf16),
        in_specs=[anywhere] * 6 + [scalar] * 3,
        out_specs=anywhere,
        scratch_shapes=[
            pltpu.VMEM((row_count, points), bf16),
            pltpu.VMEM((lanes, points, 2, width), bf16),
            pltpu.VMEM((2, n_tgt, levels, rank, 2, width), bf16),
            pltpu.VMEM((clusters, rank, 2, width), bf16),
            pltpu.VMEM((slots, width, 2, width), bf16),
            pltpu.VMEM((clusters, row_count, 2 * width), bf16),
            pltpu.VMEM((slots + 1, row_count, width), f32),
            pltpu.VMEM((n_tgt, 2, rhs // n_tgt, rank), f32),
            pltpu.VMEM((2, rhs // n_tgt, rank), f32),
            pltpu.VMEM((levels, CHUNKS, 2, rows, rank), bf16),
            pltpu.VMEM((levels, CHUNKS, 2, rows, rank), bf16),
            pltpu.VMEM((n_tgt, CHUNKS, 2, rows, rank), bf16),
            pltpu.VMEM((row_count, points), bf16),
            dma,
            dma((lanes, comp_parts)),
            dma((2,)),
            dma((2,)),
            dma((2,)),
            dma((clusters,)),
            dma((tile_parts,)),
            dma((2,)),
            dma((levels, CHUNKS)),
            dma((levels, CHUNKS)),
            dma((2, CHUNKS)),
            dma((out_parts,)),
        ],
        compiler_params=pltpu.CompilerParams(collective_id=0, has_side_effects=True),
    )(densities, compress, level_a, level_b, expand, near_tiles, tile_pairs.T, tile_count, cluster_order)


def solution(mesh):
    placed = (
        P("grp", ("src", "tgt")),
        P(("grp", "src", "tgt"), None, None),
        P("grp", "src", None, "tgt"),
        P("grp", "src", None, "tgt"),
        P(("grp", "src"), None, "tgt"),
        P(("grp", "src", "tgt"), None, None, None),
        P(("grp", "src", "tgt"), None),
        P(("grp", "src", "tgt")),
        P(("grp", "src", "tgt"), None),
    )
    return jax.shard_map(
        shards, mesh=mesh, in_specs=placed, out_specs=P("grp", ("src", "tgt")), check_vma=False
    )
```
